8 devices in a mesh: dp: 1 (over z), tp: 8 (over y, x, core).
Axes of the slice: x: 2, y: 2, z: 1, core: 2. Of those that a mesh axis runs over, the one named last changes fastest.
Arguments:
- x: bfloat16 [32, 256, 1536], P('dp', 'tp')
- d_out: bfloat16 [32, 256, 1536], P('dp', 'tp')
- ln1_gain: float32 [1536], replicated
- ln1_bias: float32 [1536], replicated
- w_q: bfloat16 [1536, 16, 96], P(None, 'tp')
- b_q: bfloat16 [16, 96], P('tp')
- w_k: bfloat16 [1536, 16, 96], P(None, 'tp')
- w_v: bfloat16 [1536, 16, 96], P(None, 'tp')
- b_v: bfloat16 [16, 96], P('tp')
- w_o: bfloat16 [16, 96, 1536], P('tp')
- b_o: bfloat16 [1536], replicated
- ln2_gain: float32 [1536], replicated
- ln2_bias: float32 [1536], replicated
- w_1: bfloat16 [1536, 6144], P(None, 'tp')
- b_1: bfloat16 [6144], P('tp')
- w_2: bfloat16 [6144, 1536], P('tp')
- b_2: bfloat16 [1536], replicated
Outputs:
- output 1: bfloat16 [32, 256, 1536], P('dp', 'tp')
- output 2: bfloat16 [32, 256, 1536], P('dp', 'tp')
- output 3: float32 [1536], P('dp')
- output 4: float32 [1536], P('dp')
- output 5: bfloat16 [1536, 16, 96], P('dp', 'tp')
- output 6: bfloat16 [16, 96], P(('dp', 'tp'))
- output 7: bfloat16 [1536, 16, 96], P('dp', 'tp')
- output 8: bfloat16 [1536, 16, 96], P('dp', 'tp')
- output 9: bfloat16 [16, 96], P(('dp', 'tp'))
- output 10: bfloat16 [16, 96, 1536], P(('dp', 'tp'))
- output 11: bfloat16 [1536], P('dp')
- output 12: float32 [1536], P('dp')
- output 13: float32 [1536], P('dp')
- output 14: bfloat16 [1536, 6144], P('dp', 'tp')
- output 15: bfloat16 [6144], P(('dp', 'tp'))
- output 16: bfloat16 [6144, 1536], P(('dp', 'tp'))
- output 17: bfloat16 [1536], P('dp')
All inputs are finite; a program needn't handle non-finite values.
Results may differ from the reference program's by a relative error of at most 0.0195979.
Values are sent between devices in bfloat16 or wider.
A program may use at most 1 GiB of HBM per device.

```python
import math
import jax
import jax.numpy as jnp
from jax import lax

IMAGES = 32
PATCHES = 256
WIDTH = 1536
NUM_HEADS = 16
HEAD_DIM = 96
MLP_DIM = 6144
LN_EPS = 1e-6
ATT_SCALE = 1.0 / math.sqrt(HEAD_DIM)
TOKENS = IMAGES * PATCHES


def draw_normal(key, shape, scale):
    return jax.random.normal(key, shape, jnp.float32) * scale


def setup_inputs(seed: int = 0, part: int = 0) -> dict:
    part_key = jax.random.fold_in(jax.random.key(seed), part)
    act_keys = jax.random.split(part_key, 4)
    wt_keys = jax.random.split(jax.random.key(seed + 1), 15)
    act_shape = (IMAGES, PATCHES, WIDTH)
    row_scale = jnp.exp(draw_normal(act_keys[0], (IMAGES, PATCHES, 1), 0.5))
    row_shift = draw_normal(act_keys[1], (IMAGES, PATCHES, 1), 0.5)
    x = (draw_normal(act_keys[2], act_shape, 1.0) * row_scale + row_shift).astype(jnp.bfloat16)
    d_out = draw_normal(act_keys[3], act_shape, 1.0).astype(jnp.bfloat16)
    in_scale = WIDTH ** -0.5
    qk_scale = in_scale * math.sqrt(math.sqrt(math.log(PATCHES / 8.0)))
    head_w = (WIDTH, NUM_HEADS, HEAD_DIM)
    head_b = (NUM_HEADS, HEAD_DIM)
    return {
        'x': x,
        'd_out': d_out,
        'ln1_gain': 1.0 + draw_normal(wt_keys[0], (WIDTH,), 0.25),
        'ln1_bias': draw_normal(wt_keys[1], (WIDTH,), 0.3),
        'w_q': draw_normal(wt_keys[2], head_w, qk_scale).astype(jnp.bfloat16),
        'b_q': draw_normal(wt_keys[3], head_b, 0.5).astype(jnp.bfloat16),
        'w_k': draw_normal(wt_keys[4], head_w, qk_scale).astype(jnp.bfloat16),
        'w_v': draw_normal(wt_keys[5], head_w, in_scale).astype(jnp.bfloat16),
        'b_v': draw_normal(wt_keys[6], head_b, 0.5).astype(jnp.bfloat16),
        'w_o': draw_normal(wt_keys[7], (NUM_HEADS, HEAD_DIM, WIDTH), 2.5 * in_scale).astype(jnp.bfloat16),
        'b_o': draw_normal(wt_keys[8], (WIDTH,), 0.5).astype(jnp.bfloat16),
        'ln2_gain': 1.0 + draw_normal(wt_keys[9], (WIDTH,), 0.25),
        'ln2_bias': draw_normal(wt_keys[10], (WIDTH,), 0.3),
        'w_1': draw_normal(wt_keys[11], (WIDTH, MLP_DIM), in_scale).astype(jnp.bfloat16),
        'b_1': draw_normal(wt_keys[12], (MLP_DIM,), 0.5).astype(jnp.bfloat16),
        'w_2': draw_normal(wt_keys[13], (MLP_DIM, WIDTH), 1.5 * MLP_DIM ** -0.5).astype(jnp.bfloat16),
        'b_2': draw_normal(wt_keys[14], (WIDTH,), 0.5).astype(jnp.bfloat16),
    }


def layer_norm(rows, ln_gain, ln_bias):
    row_mean = jnp.mean(rows, axis=-1, keepdims=True)
    centered = rows - row_mean
    variance = jnp.mean(centered * centered, axis=-1, keepdims=True)
    return centered * lax.rsqrt(variance + LN_EPS) * ln_gain + ln_bias


def attend_image(qkv_image):
    queries, keys, values = qkv_image
    scores = jnp.einsum('qhd,khd->hqk', queries.astype(jnp.float32), keys.astype(jnp.float32)) * ATT_SCALE
    probs = jax.nn.softmax(scores, axis=-1).astype(jnp.bfloat16)
    mixed = jnp.einsum('hqk,khd->qhd', probs.astype(jnp.float32), values.astype(jnp.float32))
    return mixed.astype(jnp.bfloat16)


def forward(x, ln1_gain, ln1_bias, w_q, b_q, w_k, w_v, b_v, w_o, b_o, ln2_gain, ln2_bias, w_1, b_1, w_2, b_2):
    x_f32 = x.reshape(TOKENS, WIDTH).astype(jnp.float32)
    h_one = layer_norm(x_f32, ln1_gain, ln1_bias).astype(jnp.bfloat16)
    w_qkv = jnp.concatenate([w_q.reshape(WIDTH, WIDTH), w_k.reshape(WIDTH, WIDTH), w_v.reshape(WIDTH, WIDTH)], axis=1)
    b_qkv = jnp.concatenate([b_q.reshape(WIDTH).astype(jnp.float32), jnp.zeros((WIDTH,), jnp.float32), b_v.reshape(WIDTH).astype(jnp.float32)])
    qkv = (jnp.dot(h_one, w_qkv, preferred_element_type=jnp.float32) + b_qkv).astype(jnp.bfloat16)
    head_shape = (IMAGES, PATCHES, NUM_HEADS, HEAD_DIM)
    queries = qkv[:, :WIDTH].reshape(head_shape)
    keys = qkv[:, WIDTH:2 * WIDTH].reshape(head_shape)
    values = qkv[:, 2 * WIDTH:].reshape(head_shape)
    mixed = lax.map(attend_image, (queries, keys, values)).reshape(TOKENS, WIDTH)
    attn_out = jnp.dot(mixed, w_o.reshape(WIDTH, WIDTH), preferred_element_type=jnp.float32)
    x_mid = (x_f32 + attn_out + b_o).astype(jnp.bfloat16)
    mid_f32 = x_mid.astype(jnp.float32)
    h_two = layer_norm(mid_f32, ln2_gain, ln2_bias).astype(jnp.bfloat16)
    pre_act = (jnp.dot(h_two, w_1, preferred_element_type=jnp.float32) + b_1).astype(jnp.bfloat16)
    hidden = jax.nn.gelu(pre_act.astype(jnp.float32), approximate=True).astype(jnp.bfloat16)
    mlp_out = jnp.dot(hidden, w_2, preferred_element_type=jnp.float32)
    y_out = (mid_f32 + mlp_out + b_2).astype(jnp.bfloat16)
    return y_out.reshape(IMAGES, PATCHES, WIDTH)


def reference(x, d_out, ln1_gain, ln1_bias, w_q, b_q, w_k, w_v, b_v, w_o, b_o, ln2_gain, ln2_bias, w_1, b_1, w_2, b_2):
    y_out, pullback = jax.vjp(forward, x, ln1_gain, ln1_bias, w_q, b_q, w_k, w_v, b_v, w_o, b_o, ln2_gain, ln2_bias, w_1, b_1, w_2, b_2)
    (grad_x, grad_ln1_gain, grad_ln1_bias, grad_w_q, grad_b_q, grad_w_k, grad_w_v, grad_b_v, grad_w_o, grad_b_o,
     grad_ln2_gain, grad_ln2_bias, grad_w_1, grad_b_1, grad_w_2, grad_b_2) = pullback(d_out)
    return (y_out, grad_x, grad_ln1_gain, grad_ln1_bias, grad_w_q, grad_b_q, grad_w_k, grad_w_v, grad_b_v, grad_w_o, grad_b_o,
            grad_ln2_gain, grad_ln2_bias, grad_w_1, grad_b_1, grad_w_2, grad_b_2)
```

```python
import functools
import math
import jax
import jax.numpy as jnp
from jax import lax
from jax.experimental import pallas as pl
from jax.experimental.pallas import tpu as pltpu
from jax.sharding import Mesh, PartitionSpec as P

LN_EPS = 1e-6
BF = jnp.bfloat16
F32 = jnp.float32


def layer_norm(rows, ln_gain, ln_bias):
    row_mean = jnp.mean(rows, axis=-1, keepdims=True)
    centered = rows - row_mean
    variance = jnp.mean(centered * centered, axis=-1, keepdims=True)
    return centered * lax.rsqrt(variance + LN_EPS) * ln_gain + ln_bias


def gelu_tanh(pre_act):
    return jax.nn.gelu(pre_act, approximate=True)


HEADS_PER_STEP = 4


def head_cols(head, which, heads, hd):
    dev, h = divmod(head, heads)
    start = (dev * 3 + which) * heads * hd + h * hd
    return slice(start, start + hd)


def probs_of(q, k, scale):
    s = lax.dot_general(q, k, (((1,), (1,)), ((), ())), preferred_element_type=F32) * scale
    e = jnp.exp(s - jnp.max(s, axis=-1, keepdims=True))
    return e / jnp.sum(e, axis=-1, keepdims=True)


def attn_fwd_kernel(heads, hd, qkv_ref, out_ref):
    scale = 1.0 / math.sqrt(hd)
    outs = []
    qkv = qkv_ref[...]
    for head in range(HEADS_PER_STEP):
        q, k, v = (qkv[:, head_cols(head, i, heads, hd)] for i in range(3))
        p = probs_of(q, k, scale).astype(BF)
        outs.append(dot_nn(p, v).astype(BF))
    out_ref[...] = jnp.concatenate(outs, axis=1)


def attn_bwd_kernel(heads, hd, qkv_ref, da_ref, out_ref):
    scale = 1.0 / math.sqrt(hd)
    pieces = {}
    qkv, d_mixed = qkv_ref[...], da_ref[...]
    for head in range(HEADS_PER_STEP):
        q, k, v = (qkv[:, head_cols(head, i, heads, hd)] for i in range(3))
        da = d_mixed[:, head * hd:(head + 1) * hd]
        p = probs_of(q, k, scale)
        dv = dot_tn(p.astype(BF), da)
        dp = dot_nt(da, v).astype(BF).astype(F32)
        ds = p * (dp - jnp.sum(dp * p, axis=-1, keepdims=True))
        ds = (ds * scale).astype(BF)
        grads = (dot_nn(ds, k), dot_tn(ds, q), dv)
        for i in range(3):
            pieces[head_cols(head, i, heads, hd).start] = grads[i].astype(BF)
    out_ref[...] = jnp.concatenate([pieces[c] for c in sorted(pieces)], axis=1)


def attention_call(body, images, tokens, out_cols, args, hd, flops):
    steps = args[0].shape[1] // (3 * hd * HEADS_PER_STEP)

    def spec(cols):
        return pl.BlockSpec((tokens, cols // steps), lambda b, g: (b, g))

    return pl.pallas_call(
        body, grid=(images, steps),
        in_specs=[spec(a.shape[1]) for a in args], out_specs=spec(out_cols),
        out_shape=jax.ShapeDtypeStruct((images * tokens, out_cols), BF),
        compiler_params=pltpu.CompilerParams(dimension_semantics=('parallel', 'parallel')),
        cost_estimate=pl.CostEstimate(flops=flops, transcendentals=0,
                                      bytes_accessed=2 * images * tokens * (out_cols + sum(a.shape[1] for a in args))),
    )(*args)


def dot_nt(a, b):
    return lax.dot_general(a, b, (((1,), (1,)), ((), ())), preferred_element_type=F32)


def dot_nn(a, b):
    return lax.dot_general(a, b, (((1,), (0,)), ((), ())), preferred_element_type=F32)


def dot_tn(a, b):
    return lax.dot_general(a, b, (((0,), (0,)), ((), ())), preferred_element_type=F32)


def row_sum(rows):
    return jnp.sum(rows, axis=0, dtype=F32)


def solution(mesh):
    chips = mesh.shape['tp'] // 2
    mesh = Mesh(mesh.devices.reshape(mesh.shape['dp'], chips, 2), ('dp', 'chip', 'core'))
    TP = ('chip', 'core')
    act_spec = P('dp', TP, None)
    replicated = P()
    head_w = P(None, TP, None)
    head_b = P(TP, None)
    grad_head_w = P('dp', TP, None)
    grad_head_b = P(('dp',) + TP, None)
    grad_vec = P('dp')
    in_specs = (act_spec, act_spec, replicated, replicated, head_w, head_b, head_w, head_w, head_b,
                P(TP, None, None), replicated, replicated, replicated, P(None, TP), P(TP), P(TP, None), replicated)
    out_specs = (act_spec, act_spec, grad_vec, grad_vec, grad_head_w, grad_head_b, grad_head_w, grad_head_w, grad_head_b,
                 P(('dp',) + TP, None, None), grad_vec, grad_vec, grad_vec, P('dp', TP), P(('dp',) + TP),
                 P(('dp',) + TP, None), grad_vec)
    tp = chips * 2

    def gather(rows, axes=('core', 'chip')):
        return lax.all_gather(rows, axes, axis=0, tiled=True)

    def weight_grad(cotangent, acts):
        core = lax.axis_index('core')
        half = cotangent.shape[1] // 2

        def part(which):
            return dot_tn(lax.dynamic_slice_in_dim(cotangent, which * half, half, axis=1), acts)

        other = lax.ppermute(part(1 - core), 'core', [(0, 1), (1, 0)])
        own = part(core) + other
        return lax.psum_scatter(own, 'chip', scatter_dimension=0, tiled=True).astype(BF)

    def to_images(rows):
        return lax.all_to_all(rows, TP, 0, 1, tiled=True)

    def to_tokens(rows):
        me = lax.axis_index(TP)
        img, toks, width = rows.shape
        toks //= tp

        def piece(dev):
            return lax.dynamic_slice_in_dim(rows, dev * toks, toks, axis=1)

        out = jnp.zeros((img * tp, toks, width), rows.dtype)
        out = lax.dynamic_update_slice_in_dim(out, piece(me), me * img, axis=0)
        for k in range(1, tp):
            got = lax.ppermute(piece(me ^ k), TP, [(i, i ^ k) for i in range(tp)])
            out = lax.dynamic_update_slice_in_dim(out, got, (me ^ k) * img, axis=0)
        return out

    def layer_step(x, d_out, ln1_gain, ln1_bias, w_q, b_q, w_k, w_v, b_v, w_o, b_o, ln2_gain, ln2_bias, w_1, b_1, w_2, b_2):
        images, toks, width = x.shape
        heads, hd = w_q.shape[1], w_q.shape[2]
        img = images // tp
        rows = img * toks * tp
        lw = heads * hd
        me = lax.axis_index(TP)
        me_cc = lax.axis_index(('core', 'chip'))

        def head_rows(w):
            return w.transpose(1, 2, 0).reshape(lw, width)

        w_qkv = gather(jnp.concatenate([head_rows(w_q), head_rows(w_k), head_rows(w_v)], axis=0))

        def bias_rows(bias):
            return bias.astype(F32).reshape(-1, hd)

        b_own = jnp.concatenate([bias_rows(b_q), jnp.zeros((heads, hd), F32), bias_rows(b_v), bias_rows(b_1)], axis=0)
        b_rows = lax.all_gather(b_own, ('core', 'chip'), axis=0, tiled=False)
        b_qkv = b_rows[:, :3 * heads].reshape(3 * lw * tp)
        b_1all = b_rows[:, 3 * heads:].reshape(b_1.shape[0] * tp)
        w_oall = gather(w_o.reshape(lw, width))
        w_1all = gather(w_1.T)
        w_2all = gather(w_2)
        d_out_all = gather(d_out, TP)

        x_img = to_images(x).reshape(rows, width)
        x_f32 = x_img.astype(F32)
        h_one_f, ln1_pull = jax.vjp(layer_norm, x_f32, ln1_gain, ln1_bias)
        h_one = h_one_f.astype(BF)
        qkv = (dot_nt(h_one, w_qkv) + b_qkv.astype(F32)).astype(BF)
        attn_flops = 4 * rows * toks * tp * tp * lw
        mixed_rows = attention_call(functools.partial(attn_fwd_kernel, heads, hd), img, toks * tp,
                                    tp * lw, (qkv,), hd, attn_flops)
        x_mid = (x_f32 + dot_nn(mixed_rows, w_oall) + b_o.astype(F32)).astype(BF)
        mid_f32 = x_mid.astype(F32)
        h_two_f, ln2_pull = jax.vjp(layer_norm, mid_f32, ln2_gain, ln2_bias)
        h_two = h_two_f.astype(BF)
        h_two_all = gather(h_two, TP)

        pre_act = (dot_nt(h_two, w_1all) + b_1all.astype(F32)).astype(BF)
        hidden_f, gelu_pull = jax.vjp(gelu_tanh, pre_act.astype(F32))
        hidden = hidden_f.astype(BF)
        y_img = (mid_f32 + dot_nn(hidden, w_2all) + b_2.astype(F32)).astype(BF)
        y_out = to_tokens(y_img.reshape(img, toks * tp, width))
        d_stack = d_out_all.reshape(tp, images, toks, width)
        d_img = lax.dynamic_slice_in_dim(d_stack, me * img, img, axis=1).transpose(1, 0, 2, 3).reshape(rows, width)
        d_hidden = lax.optimization_barrier(dot_nt(d_img, w_2all).astype(BF))
        (d_pre_f,) = gelu_pull(d_hidden.astype(F32))
        d_pre = d_pre_f.astype(BF)
        d_h_two = dot_nn(d_pre, w_1all).astype(BF)
        d_mid_ln, g_ln2_gain, g_ln2_bias = ln2_pull(d_h_two.astype(F32))
        d_mid = (d_img.astype(F32) + d_mid_ln).astype(BF)
        d_mixed = dot_nt(d_mid, w_oall).astype(BF)
        grad_w_o = weight_grad(mixed_rows, d_mid).reshape(w_o.shape)
        d_qkv = attention_call(functools.partial(attn_bwd_kernel, heads, hd), img, toks * tp,
                               3 * tp * lw, (qkv, d_mixed), hd, 5 * attn_flops // 2)
        part_b_qkv = row_sum(d_qkv)
        grad_w_qkv = weight_grad(d_qkv, h_one).reshape(3, heads, hd, width)
        grad_w_q, grad_w_k, grad_w_v = (grad_w_qkv[i].transpose(2, 0, 1) for i in range(3))
        d_h_one = dot_nn(d_qkv, w_qkv).astype(BF)
        d_in_ln, g_ln1_gain, g_ln1_bias = ln1_pull(d_h_one.astype(F32))
        grad_x_img = (d_mid.astype(F32) + d_in_ln).astype(BF)
        grad_x = to_tokens(grad_x_img.reshape(img, toks * tp, width))

        t_pre = (dot_nn(h_two_all, w_1) + b_1.astype(F32)).astype(BF)
        t_hidden_f, t_pull = jax.vjp(gelu_tanh, t_pre.astype(F32))
        t_hidden = t_hidden_f.astype(BF)
        d_ord = d_stack.transpose(1, 0, 2, 3).reshape(images * tp * toks, width)
        t_d_hidden = lax.optimization_barrier(dot_nt(d_ord, w_2).astype(BF))
        (t_d_pre_f,) = t_pull(t_d_hidden.astype(F32))
        t_d_pre = t_d_pre_f.astype(BF)
        grad_b_1 = row_sum(t_d_pre).astype(BF)
        grad_w_1 = dot_tn(h_two_all, t_d_pre).astype(BF)
        grad_w_2 = dot_tn(t_hidden, d_ord).astype(BF)
        vec_parts = jnp.concatenate([g_ln1_gain, g_ln1_bias, row_sum(d_mid), g_ln2_gain, g_ln2_bias, row_sum(d_img), part_b_qkv])
        vec_parts, grad_w_1, grad_w_2 = lax.optimization_barrier((vec_parts, grad_w_1, grad_w_2))
        vec_sums = lax.psum(vec_parts.reshape(9, width), TP).reshape(9 * width)
        grad_b_qkv = lax.dynamic_slice_in_dim(vec_sums[6 * width:], me_cc * 3 * lw, 3 * lw).astype(BF).reshape(3, heads, hd)
        vec_sums = vec_sums[:6 * width].reshape(6, width)
        return (y_out, grad_x, vec_sums[0], vec_sums[1], grad_w_q, grad_b_qkv[0], grad_w_k, grad_w_v, grad_b_qkv[2], grad_w_o,
                vec_sums[2].astype(BF), vec_sums[3], vec_sums[4], grad_w_1, grad_b_1, grad_w_2,
                vec_sums[5].astype(BF))

    return jax.shard_map(layer_step, mesh=mesh, in_specs=in_specs, out_specs=out_specs, check_vma=False)
```

```python
import functools
import math
import jax
import jax.numpy as jnp
from jax import lax
from jax.experimental import pallas as pl
from jax.experimental.pallas import tpu as pltpu
from jax.sharding import Mesh, PartitionSpec as P

LN_EPS = 1e-6
BF = jnp.bfloat16
F32 = jnp.float32


def layer_norm(rows, ln_gain, ln_bias):
    row_mean = jnp.mean(rows, axis=-1, keepdims=True)
    centered = rows - row_mean
    variance = jnp.mean(centered * centered, axis=-1, keepdims=True)
    return centered * lax.rsqrt(variance + LN_EPS) * ln_gain + ln_bias


HEADS_PER_STEP = 4


def head_cols(head, which, heads, hd):
    dev, h = divmod(head, heads)
    start = (dev * 3 + which) * heads * hd + h * hd
    return slice(start, start + hd)


def probs_of(q, k, scale):
    s = lax.dot_general(q, k, (((1,), (1,)), ((), ())), preferred_element_type=F32) * scale
    e = jnp.exp(s - jnp.max(s, axis=-1, keepdims=True))
    return e * (1.0 / jnp.sum(e, axis=-1, keepdims=True))


def attn_fwd_kernel(heads, hd, qkv_ref, out_ref):
    scale = 1.0 / math.sqrt(hd)
    outs = []
    qkv = qkv_ref[...]
    for head in range(HEADS_PER_STEP):
        q, k, v = (qkv[:, head_cols(head, i, heads, hd)] for i in range(3))
        p = probs_of(q, k, scale).astype(BF)
        outs.append(dot_nn(p, v).astype(BF))
    out_ref[...] = jnp.concatenate(outs, axis=1)


def attn_bwd_kernel(heads, hd, qkv_ref, da_ref, out_ref):
    scale = 1.0 / math.sqrt(hd)
    pieces = {}
    qkv, d_mixed = qkv_ref[...], da_ref[...]
    for head in range(HEADS_PER_STEP):
        q, k, v = (qkv[:, head_cols(head, i, heads, hd)] for i in range(3))
        da = d_mixed[:, head * hd:(head + 1) * hd]
        p = probs_of(q, k, scale)
        dv = dot_tn(p.astype(BF), da)
        dp = dot_nt(da, v).astype(BF).astype(F32)
        ds = p * (dp - jnp.sum(dp * p, axis=-1, keepdims=True))
        ds = (ds * scale).astype(BF)
        grads = (dot_nn(ds, k), dot_tn(ds, q), dv)
        for i in range(3):
            pieces[head_cols(head, i, heads, hd).start] = grads[i].astype(BF)
    out_ref[...] = jnp.concatenate([pieces[c] for c in sorted(pieces)], axis=1)


def attention_call(body, images, tokens, out_cols, args, hd, flops):
    steps = args[0].shape[1] // (3 * hd * HEADS_PER_STEP)

    def spec(cols):
        return pl.BlockSpec((tokens, cols // steps), lambda b, g: (b, g))

    return pl.pallas_call(
        body, grid=(images, steps),
        in_specs=[spec(a.shape[1]) for a in args], out_specs=spec(out_cols),
        out_shape=jax.ShapeDtypeStruct((images * tokens, out_cols), BF),
        compiler_params=pltpu.CompilerParams(dimension_semantics=('parallel', 'parallel')),
        cost_estimate=pl.CostEstimate(flops=flops, transcendentals=0,
                                      bytes_accessed=2 * images * tokens * (out_cols + sum(a.shape[1] for a in args))),
    )(*args)


def gelu_both(x, d_hid):
    c = math.sqrt(2.0 / math.pi)
    x2 = x * x
    t = jnp.tanh(c * (x + 0.044715 * (x2 * x)))
    cdf = 0.5 * (1.0 + t)
    slope = cdf + (0.5 * c) * x * (1.0 - t * t) * (1.0 + (3 * 0.044715) * x2)
    return (x * cdf).astype(BF), (d_hid * slope).astype(BF)


def row_pass_kernel(h_ref, d_ref, w1_ref, w2_ref, b1_ref, y_ref, dh_ref):
    @pl.when(pl.program_id(1) == 0)
    def _():
        y_ref[...] = jnp.zeros_like(y_ref)
        dh_ref[...] = jnp.zeros_like(dh_ref)

    w1, w2 = w1_ref[...], w2_ref[...]
    x = (dot_nt(h_ref[...], w1) + b1_ref[...]).astype(BF).astype(F32)
    d_hid = dot_nt(d_ref[...], w2).astype(BF).astype(F32)
    hid, d_pre = gelu_both(x, d_hid)
    dh_ref[...] += dot_nn(d_pre, w1)
    y_ref[...] += dot_nn(hid, w2)


def row_pass(h, d, w_1t, w_2, b_1):
    rows, width = h.shape
    cols = w_1t.shape[0]
    rb, cb = rows // 2, 512
    row_spec = pl.BlockSpec((rb, width), lambda i, j: (i, 0))
    col_spec = pl.BlockSpec((cb, width), lambda i, j: (j, 0))
    out = jax.ShapeDtypeStruct((rows, width), F32)
    return pl.pallas_call(
        row_pass_kernel, grid=(2, cols // cb), name='row_pass',
        in_specs=[row_spec, row_spec, col_spec, col_spec, pl.BlockSpec((1, cb), lambda i, j: (0, j))],
        out_specs=[row_spec, row_spec], out_shape=[out, out],
        compiler_params=pltpu.CompilerParams(dimension_semantics=('arbitrary', 'arbitrary'), vmem_limit_bytes=60 * 2**20),
        cost_estimate=pl.CostEstimate(flops=8 * rows * width * cols, transcendentals=rows * cols, bytes_accessed=8 * cols * width),
    )(h, d, w_1t, w_2, b_1.reshape(1, cols))


def column_pass_kernel(h_ref, d_ref, w1_ref, w2_ref, b1_ref, gw1_ref, gw2_ref, gb1_ref, acc1, acc2, accb):
    step = pl.program_id(0)

    @pl.when(step == 0)
    def _():
        acc1[...] = jnp.zeros_like(acc1)
        acc2[...] = jnp.zeros_like(acc2)
        accb[...] = jnp.zeros_like(accb)

    width = h_ref.shape[1]
    h = h_ref[...]
    d = jnp.concatenate([d_ref[:, i].reshape(-1, width) for i in range(d_ref.shape[1])], axis=0)
    x = (dot_nn(h, w1_ref[...]) + b1_ref[...]).astype(BF).astype(F32)
    d_hid = dot_nt(d, w2_ref[...]).astype(BF).astype(F32)
    hid, d_pre = gelu_both(x, d_hid)
    accb[...] += jnp.sum(d_pre.astype(F32), axis=0, keepdims=True)
    acc1[...] += dot_tn(h, d_pre)
    acc2[...] += dot_tn(hid, d)

    @pl.when(step == pl.num_programs(0) - 1)
    def _():
        gw1_ref[...] = acc1[...].astype(BF)
        gw2_ref[...] = acc2[...].astype(BF)
        gb1_ref[...] = accb[...]


def column_pass(h_all, d_stack, w_1, w_2, b_1):
    tp, images, toks, width = d_stack.shape
    cols = w_1.shape[1]
    per = 2
    whole = lambda i: (0, 0)
    return pl.pallas_call(
        column_pass_kernel, grid=(images // per,), name='column_pass',
        in_specs=[pl.BlockSpec((per * tp * toks, width), lambda i: (i, 0)), pl.BlockSpec((tp, per, toks, width), lambda i: (0, i, 0, 0)),
                  pl.BlockSpec((width, cols), whole), pl.BlockSpec((cols, width), whole), pl.BlockSpec((1, cols), whole)],
        out_specs=[pl.BlockSpec((width, cols), whole), pl.BlockSpec((cols, width), whole), pl.BlockSpec((1, cols), whole)],
        out_shape=[jax.ShapeDtypeStruct((width, cols), BF), jax.ShapeDtypeStruct((cols, width), BF), jax.ShapeDtypeStruct((1, cols), F32)],
        scratch_shapes=[pltpu.VMEM((width, cols), F32), pltpu.VMEM((cols, width), F32), pltpu.VMEM((1, cols), F32)],
        compiler_params=pltpu.CompilerParams(dimension_semantics=('arbitrary',), vmem_limit_bytes=60 * 2**20),
        cost_estimate=pl.CostEstimate(flops=8 * h_all.shape[0] * width * cols, transcendentals=h_all.shape[0] * cols,
                                      bytes_accessed=4 * h_all.size),
    )(h_all, d_stack, w_1, w_2, b_1.astype(F32).reshape(1, cols))


def dot_nt(a, b):
    return lax.dot_general(a, b, (((1,), (1,)), ((), ())), preferred_element_type=F32)


def dot_nn(a, b):
    return lax.dot_general(a, b, (((1,), (0,)), ((), ())), preferred_element_type=F32)


def dot_tn(a, b):
    return lax.dot_general(a, b, (((0,), (0,)), ((), ())), preferred_element_type=F32)


def row_sum(rows):
    return jnp.sum(rows, axis=0, dtype=F32)


def solution(mesh):
    chips = mesh.shape['tp'] // 2
    mesh = Mesh(mesh.devices.reshape(mesh.shape['dp'], chips, 2), ('dp', 'chip', 'core'))
    TP = ('chip', 'core')
    act_spec = P('dp', TP, None)
    replicated = P()
    head_w = P(None, TP, None)
    head_b = P(TP, None)
    grad_head_w = P('dp', TP, None)
    grad_head_b = P(('dp',) + TP, None)
    grad_vec = P('dp')
    in_specs = (act_spec, act_spec, replicated, replicated, head_w, head_b, head_w, head_w, head_b,
                P(TP, None, None), replicated, replicated, replicated, P(None, TP), P(TP), P(TP, None), replicated)
    out_specs = (act_spec, act_spec, grad_vec, grad_vec, grad_head_w, grad_head_b, grad_head_w, grad_head_w, grad_head_b,
                 P(('dp',) + TP, None, None), grad_vec, grad_vec, grad_vec, P('dp', TP), P(('dp',) + TP),
                 P(('dp',) + TP, None), grad_vec)
    tp = chips * 2

    def gather(rows, axes=('core', 'chip')):
        return lax.all_gather(rows, axes, axis=0, tiled=True)

    X_PAIR = [(c, c ^ 1) for c in range(chips)]
    Y_PAIR = [(c, c ^ 2) for c in range(chips)]
    CORES = [(0, 1), (1, 0)]

    def gather_near(rows):
        half = rows.shape[0] // 2
        from_x = lax.ppermute(rows, 'chip', X_PAIR)
        from_y = lax.ppermute(rows, 'chip', Y_PAIR)
        far_top = lax.ppermute(from_x[:half], 'chip', Y_PAIR)
        far_bot = lax.ppermute(from_y[half:], 'chip', X_PAIR)
        own = [rows, from_x, from_y, far_top, far_bot]
        return jnp.concatenate(own + [lax.ppermute(r, 'core', CORES) for r in own], axis=0)

    def near_order(rows):
        chip, core = lax.axis_index('chip'), lax.axis_index('core')
        return jnp.concatenate([lax.dynamic_slice_in_dim(rows, (core ^ p) * chips + (chip ^ k), 1, axis=0)
                                for p in range(2) for k in range(chips)], axis=0)

    def weight_grad(cotangent, acts):
        core = lax.axis_index('core')
        half = cotangent.shape[1] // 2

        def part(which):
            return dot_tn(lax.dynamic_slice_in_dim(cotangent, which * half, half, axis=1), acts)

        other = lax.ppermute(part(1 - core), 'core', [(0, 1), (1, 0)])
        return part(core) + other

    def scatter(own):
        chip = lax.axis_index('chip')
        n = own.shape[0] // chips
        h = n // 2

        def piece(k, low):
            return lax.dynamic_slice_in_dim(own, (chip ^ k) * n + low * h, h, axis=0)

        top3, bot3, top1, bot2, top0, bot0 = lax.optimization_barrier(
            (piece(3, 0), piece(3, 1), piece(1, 0), piece(2, 1), piece(0, 0), piece(0, 1)))
        far_top = lax.ppermute(top3, 'chip', X_PAIR)
        far_bot = lax.ppermute(bot3, 'chip', Y_PAIR)
        x_top = lax.ppermute(top1, 'chip', X_PAIR)
        y_bot = lax.ppermute(bot2, 'chip', Y_PAIR)
        x_bot = lax.ppermute(piece(1, 1) + far_bot, 'chip', X_PAIR)
        y_top = lax.ppermute(piece(2, 0) + far_top, 'chip', Y_PAIR)
        return jnp.concatenate([top0 + x_top + y_top, bot0 + x_bot + y_bot], axis=0).astype(BF), top3

    def to_images(rows):
        return lax.all_to_all(rows, TP, 0, 1, tiled=True)

    def to_tokens(rows):
        me = lax.axis_index(TP)
        img, toks, width = rows.shape
        toks //= tp

        def piece(dev):
            return lax.dynamic_slice_in_dim(rows, dev * toks, toks, axis=1)

        out = jnp.zeros((img * tp, toks, width), rows.dtype)
        out = lax.dynamic_update_slice_in_dim(out, piece(me), me * img, axis=0)
        for k in range(1, tp):
            got = lax.ppermute(piece(me ^ k), TP, [(i, i ^ k) for i in range(tp)])
            out = lax.dynamic_update_slice_in_dim(out, got, (me ^ k) * img, axis=0)
        return out

    def layer_step(x, d_out, ln1_gain, ln1_bias, w_q, b_q, w_k, w_v, b_v, w_o, b_o, ln2_gain, ln2_bias, w_1, b_1, w_2, b_2):
        images, toks, width = x.shape
        heads, hd = w_q.shape[1], w_q.shape[2]
        img = images // tp
        rows = img * toks * tp
        lw = heads * hd
        me = lax.axis_index(TP)
        me_cc = lax.axis_index(('core', 'chip'))

        def head_rows(w):
            return w.transpose(1, 2, 0).reshape(lw, width)

        w_qkv = gather(jnp.concatenate([head_rows(w_q), head_rows(w_k), head_rows(w_v)], axis=0))

        def bias_rows(bias):
            return bias.astype(F32).reshape(-1, hd)

        b_own = jnp.concatenate([bias_rows(b_q), jnp.zeros((heads, hd), F32), bias_rows(b_v), bias_rows(b_1)], axis=0)
        b_rows = lax.all_gather(b_own, ('core', 'chip'), axis=0, tiled=False)
        b_qkv = b_rows[:, :3 * heads].reshape(3 * lw * tp)
        b_1all = near_order(b_rows)[:, 3 * heads:].reshape(b_1.shape[0] * tp)
        w_oall = gather(w_o.reshape(lw, width))
        w_1all = gather_near(w_1.T)
        w_2all = gather_near(w_2)
        d_out_all = gather(d_out, TP)

        x_img = to_images(x).reshape(rows, width)
        x_f32 = x_img.astype(F32)
        h_one_f, ln1_pull = jax.vjp(layer_norm, x_f32, ln1_gain, ln1_bias)
        h_one = h_one_f.astype(BF)
        qkv = (dot_nt(h_one, w_qkv) + b_qkv.astype(F32)).astype(BF)
        attn_flops = 4 * rows * toks * tp * tp * lw
        mixed_rows = attention_call(functools.partial(attn_fwd_kernel, heads, hd), img, toks * tp,
                                    tp * lw, (qkv,), hd, attn_flops)
        x_mid = (x_f32 + dot_nn(mixed_rows, w_oall) + b_o.astype(F32)).astype(BF)
        mid_f32 = x_mid.astype(F32)
        h_two_f, ln2_pull = jax.vjp(layer_norm, mid_f32, ln2_gain, ln2_bias)
        h_two = h_two_f.astype(BF)
        h_two_all = gather(h_two, TP)

        d_stack = d_out_all.reshape(tp, images, toks, width)
        d_img = lax.dynamic_slice_in_dim(d_stack, me * img, img, axis=1).transpose(1, 0, 2, 3).reshape(rows, width)
        y_part, d_h_two = row_pass(h_two, d_img, w_1all, w_2all, b_1all)
        y_img = (mid_f32 + y_part + b_2.astype(F32)).astype(BF)
        y_out = to_tokens(y_img.reshape(img, toks * tp, width))
        d_h_two = d_h_two.astype(BF)
        d_mid_ln, g_ln2_gain, g_ln2_bias = ln2_pull(d_h_two.astype(F32))
        d_mid = (d_img.astype(F32) + d_mid_ln).astype(BF)
        d_mixed = dot_nt(d_mid, w_oall).astype(BF)
        own_o = weight_grad(mixed_rows, d_mid)
        d_mixed, own_o = lax.optimization_barrier((d_mixed, own_o))
        grad_w_o, _ = scatter(own_o)
        grad_w_o = grad_w_o.reshape(w_o.shape)
        d_qkv = attention_call(functools.partial(attn_bwd_kernel, heads, hd), img, toks * tp,
                               3 * tp * lw, (qkv, d_mixed), hd, 5 * attn_flops // 2)
        part_b_qkv = row_sum(d_qkv)
        own_qkv = weight_grad(d_qkv, h_one)
        grad_w_qkv, sent = scatter(own_qkv)
        grad_w_qkv = grad_w_qkv.reshape(3, heads, hd, width)
        grad_w_q, grad_w_k, grad_w_v = (grad_w_qkv[i].transpose(2, 0, 1) for i in range(3))
        d_h_one = dot_nn(d_qkv, w_qkv).astype(BF)
        d_h_one, _ = lax.optimization_barrier((d_h_one, sent))
        d_in_ln, g_ln1_gain, g_ln1_bias = ln1_pull(d_h_one.astype(F32))
        grad_x_img = (d_mid.astype(F32) + d_in_ln).astype(BF)
        grad_x = to_tokens(grad_x_img.reshape(img, toks * tp, width))

        h_two_all, own_qkv = lax.optimization_barrier((h_two_all, own_qkv))
        grad_w_1, grad_w_2, grad_b_1 = column_pass(h_two_all, d_stack, w_1, w_2, b_1)
        grad_b_1 = grad_b_1.reshape(b_1.shape).astype(BF)
        vec_parts = jnp.concatenate([g_ln1_gain, g_ln1_bias, row_sum(d_mid), g_ln2_gain, g_ln2_bias, row_sum(d_img), part_b_qkv])
        vec_rows = jnp.pad(vec_parts.reshape(9, width), ((0, 15), (0, 0)))
        vec_rows = lax.all_gather(vec_rows, TP, axis=0, tiled=False)
        vec_sums = jnp.sum(vec_rows[:, :9], axis=0).reshape(9 * width)
        grad_b_qkv = lax.dynamic_slice_in_dim(vec_sums[6 * width:], me_cc * 3 * lw, 3 * lw).astype(BF).reshape(3, heads, hd)
        vec_sums = vec_sums[:6 * width].reshape(6, width)
        return (y_out, grad_x, vec_sums[0], vec_sums[1], grad_w_q, grad_b_qkv[0], grad_w_k, grad_w_v, grad_b_qkv[2], grad_w_o,
                vec_sums[2].astype(BF), vec_sums[3], vec_sums[4], grad_w_1, grad_b_1, grad_w_2,
                vec_sums[5].astype(BF))

    return jax.shard_map(layer_step, mesh=mesh, in_specs=in_specs, out_specs=out_specs, check_vma=False)
```
